32 devices in a mesh: seq: 8 (over y, x, core), head: 4 (over z).
Axes of the slice: x: 2, y: 2, z: 4, core: 2. Of those that a mesh axis runs over, the one named last changes fastest.
Arguments:
- latent: bfloat16 [8, 1024, 2048], P('seq', None, 'head'), may hold values from -6 to 6
- modulation: float32 [9, 2048], replicated, may hold values from -3 to 3
- spatial_qkv: bfloat16 [3, 2048, 2048], P(None, None, 'head')
- spatial_out: bfloat16 [2048, 2048], P('head'), may hold values from -0.125 to 0.125
- temporal_qkv: bfloat16 [3, 2048, 2048], P(None, None, 'head')
- temporal_out: bfloat16 [2048, 2048], P('head'), may hold values from -0.125 to 0.125
- hidden_weight: bfloat16 [2048, 8192], P(None, 'head'), may hold values from -0.125 to 0.125
- output_weight: bfloat16 [8192, 2048], P('head'), may hold values from -0.0625 to 0.0625
Outputs:
- block_out: bfloat16 [8, 1024, 2048], P(None, 'seq', 'head')
The draws below stay inside these ranges and needn't reach their ends.
All inputs are finite; a program needn't handle non-finite values.
Results may differ from the reference program's by a relative error of at most 0.009.
Values may be sent and summed in bfloat16 or wider, within the bound.
No kernel may reach another device: no remote copies, remote signals or barrier semaphores. Data moves between devices by JAX's collectives and lax.ppermute only.
A program may use at most 128 MiB of HBM per device.

```python
import jax
import jax.numpy as jnp
from jax import lax

D = 2048
HEADS = 32
FF = 8192
P_SIZE = 1024
HD = 64
FRAMES = 8


def projection_draw(key, salt):
    key = jax.random.fold_in(key, salt)
    first, second, third = jax.random.split(key, 3)
    spread = D ** (-0.5)
    query = jax.random.normal(first, (D, D), jnp.float32) * spread
    keys = jax.random.normal(second, (D, D), jnp.float32) * spread
    values = jax.random.normal(third, (D, D), jnp.float32) * spread
    return jnp.stack([query, keys, values]).astype(jnp.bfloat16)


def draw_spatial_qkv(key, part):
    return projection_draw(key, 11)


def draw_temporal_qkv(key, part):
    return projection_draw(key, 23)


def level_of(rng, extent, cuts, least, high):
    factor_of = 1.0
    for dim, parts in cuts:
        draws = jax.random.uniform(jax.random.fold_in(jax.random.fold_in(rng, 6), dim), (parts,), jnp.float32, least / len(cuts), high / len(cuts))
        factor_of = factor_of * jnp.repeat(jnp.exp(draws), extent[dim] // parts).reshape((-1,) + (1,) * (len(extent) - 1 - dim))
    return factor_of


def normal_values(stream_key, shape, scale, most, cuts=(), kind=jnp.bfloat16):
    drawn = jax.random.normal(stream_key, shape, jnp.float32) * scale
    if len(cuts) > 0:
        drawn = level_of(stream_key, shape, cuts, -0.22, 0.18) * drawn
    return jnp.clip(drawn, min=-most, max=most).astype(kind)


def setup_inputs(seed: int = 0) -> dict:
    arg_keys = jax.random.split(jax.random.key(seed), 9)
    return {
        "latent": normal_values(arg_keys[0], (FRAMES, P_SIZE, D), 1.0, 6.0, ((0, 8), (2, 4))),
        "modulation": normal_values(arg_keys[1], (9, D), 0.5, 3.0, (), jnp.float32),
        "spatial_qkv": draw_spatial_qkv(jax.random.fold_in(arg_keys[8], 71), 0),
        "spatial_out": normal_values(arg_keys[3], (D, D), D ** -0.5, 0.125, ((0, 4),)),
        "temporal_qkv": draw_temporal_qkv(jax.random.fold_in(arg_keys[8], 71), 0),
        "temporal_out": normal_values(arg_keys[5], (D, D), D ** -0.5, 0.125, ((0, 4),)),
        "hidden_weight": normal_values(arg_keys[6], (D, FF), D ** -0.5, 0.125, ((1, 4),)),
        "output_weight": normal_values(arg_keys[7], (FF, D), FF ** -0.5, 0.0625, ((0, 4),)),
    }


def layer_norm(values):
    average = lax.optimization_barrier(jnp.mean(values, axis=-1, keepdims=True))
    centred = values - average
    variance = lax.optimization_barrier(jnp.mean(centred * centred, axis=-1, keepdims=True))
    return centred * lax.rsqrt(variance + 1e-06)

def modulate(stream, modulation, offset):
    normed = layer_norm(stream.astype(jnp.float32))
    return (normed * (1.0 + modulation[offset + 1]) + modulation[offset]).astype(jnp.bfloat16)

def attend(query, keys, values):
    scores = jnp.einsum('glhd,gmhd->ghlm', query.astype(jnp.float32), keys.astype(jnp.float32)) * HD ** (-0.5)
    attn_weights = jax.nn.softmax(scores, axis=-1).astype(jnp.bfloat16)
    return jnp.einsum('ghlm,gmhd->glhd', attn_weights.astype(jnp.float32), values.astype(jnp.float32)).astype(jnp.bfloat16)

def project_three(normed, weights):
    return [jnp.dot(normed, weights[member], preferred_element_type=jnp.float32).astype(jnp.bfloat16) for member in range(3)]

def reference(latent, modulation, spatial_qkv, spatial_out, temporal_qkv, temporal_out, hidden_weight, output_weight):
    frames = latent.shape[0]
    patches = latent.shape[1]

    def split_heads(tensor):
        return tensor.reshape(frames, patches, HEADS, HD)
    normed = modulate(latent, modulation, 0)
    query, keys, values = [split_heads(member) for member in project_three(normed, spatial_qkv)]
    spatial = lax.map(lambda triple: attend(triple[0][None], triple[1][None], triple[2][None])[0], (query, keys, values))
    spatial = spatial.reshape(frames, patches, D)
    branch = jnp.dot(spatial, spatial_out, preferred_element_type=jnp.float32)
    stream_one = (latent.astype(jnp.float32) + modulation[2] * branch).astype(jnp.bfloat16)
    normed = modulate(stream_one, modulation, 3)
    query, keys, values = [jnp.transpose(split_heads(member), (1, 0, 2, 3)) for member in project_three(normed, temporal_qkv)]
    temporal = jnp.transpose(attend(query, keys, values), (1, 0, 2, 3)).reshape(frames, patches, D)
    branch = jnp.dot(temporal, temporal_out, preferred_element_type=jnp.float32)
    stream_two = (stream_one.astype(jnp.float32) + modulation[5] * branch).astype(jnp.bfloat16)
    normed = modulate(stream_two, modulation, 6)
    hidden = jax.nn.gelu(jnp.dot(normed, hidden_weight, preferred_element_type=jnp.float32), approximate=True).astype(jnp.bfloat16)
    branch = jnp.dot(hidden, output_weight, preferred_element_type=jnp.float32)
    return (stream_two.astype(jnp.float32) + modulation[8] * branch).astype(jnp.bfloat16)
```

```python
import functools

import jax
import jax.numpy as jnp
from jax import lax
from jax.experimental import pallas as pl
from jax.experimental.pallas import tpu as pltpu
from jax.sharding import PartitionSpec as P

HD = 64
LANES = 128


def modulate(stream, modulation, offset):
    values = stream.astype(jnp.float32)
    average = jnp.mean(values, axis=-1, keepdims=True)
    centred = values - average
    variance = jnp.mean(centred * centred, axis=-1, keepdims=True)
    normed = centred * lax.rsqrt(variance + 1e-06)
    return (normed * (1.0 + modulation[offset + 1]) + modulation[offset]).astype(jnp.bfloat16)


def spatial_kernel(query_ref, key_ref, value_ref, out_ref):
    pieces = []
    for head in range(query_ref.shape[1] // HD):
        span = slice(head * HD, (head + 1) * HD)
        query = query_ref[:, span] * jnp.bfloat16(HD ** (-0.5))
        scores = lax.dot_general(
            query, key_ref[:, span], (((1,), (1,)), ((), ())), preferred_element_type=jnp.float32
        )
        top = jnp.max(scores, axis=-1, keepdims=True)
        raised = jnp.exp(scores - top)
        total = jnp.sum(raised, axis=-1, keepdims=True)
        mixed = jnp.dot(
            raised.astype(jnp.bfloat16), value_ref[:, span], preferred_element_type=jnp.float32
        )
        pieces.append((mixed / total).astype(jnp.bfloat16))
    out_ref[...] = jnp.concatenate(pieces, axis=-1)


def spatial_attention(query, keys, values):
    tokens, width = query.shape
    rows = min(tokens, 512)
    return pl.pallas_call(
        spatial_kernel,
        grid=(width // LANES, tokens // rows),
        in_specs=[
            pl.BlockSpec((rows, LANES), lambda i, j: (j, i)),
            pl.BlockSpec((tokens, LANES), lambda i, j: (0, i)),
            pl.BlockSpec((tokens, LANES), lambda i, j: (0, i)),
        ],
        out_specs=pl.BlockSpec((rows, LANES), lambda i, j: (j, i)),
        out_shape=jax.ShapeDtypeStruct((tokens, width), jnp.bfloat16),
        name="spatial_attention",
    )(query, keys, values)


def temporal_kernel(query_ref, key_ref, value_ref, out_ref):
    _, frames, rows, width = query_ref.shape
    feature = lax.broadcasted_iota(jnp.int32, (width, LANES), 0) // HD
    member = lax.broadcasted_iota(jnp.int32, (width, LANES), 1)
    gather = jnp.where(feature == member, 1.0, 0.0).astype(jnp.bfloat16)
    feature = lax.broadcasted_iota(jnp.int32, (LANES, width), 1) // HD
    member = lax.broadcasted_iota(jnp.int32, (LANES, width), 0)
    spread = jnp.where(feature == member, 1.0, 0.0).astype(jnp.bfloat16)
    for frame in range(frames):
        query = query_ref[0, frame]
        products = jnp.concatenate([query * key_ref[0, other] for other in range(frames)], axis=0)
        scores = jnp.dot(products, gather, preferred_element_type=jnp.float32) * HD ** (-0.5)
        scores = [scores[other * rows : (other + 1) * rows] for other in range(frames)]
        top = functools.reduce(jnp.maximum, scores)
        raised = [jnp.exp(score - top) for score in scores]
        total = functools.reduce(jnp.add, raised)
        shares = jnp.concatenate([(part / total).astype(jnp.bfloat16) for part in raised], axis=0)
        spread_out = jnp.dot(shares, spread, preferred_element_type=jnp.float32)
        mixed = functools.reduce(
            jnp.add,
            [
                spread_out[other * rows : (other + 1) * rows]
                * value_ref[0, other].astype(jnp.float32)
                for other in range(frames)
            ],
        )
        out_ref[0, frame] = mixed.astype(jnp.bfloat16)


def temporal_attention(query, keys, values):
    groups, frames, rows, width = query.shape
    block = pl.BlockSpec((1, frames, rows, width), lambda i: (i, 0, 0, 0))
    return pl.pallas_call(
        temporal_kernel,
        grid=(groups,),
        in_specs=[block] * 3,
        out_specs=block,
        out_shape=jax.ShapeDtypeStruct(query.shape, jnp.bfloat16),
        name="temporal_attention",
    )(query, keys, values)


def project_three(normed, weights):
    return [
        jnp.dot(normed, weights[member], preferred_element_type=jnp.float32).astype(jnp.bfloat16)
        for member in range(3)
    ]


def whole_weight(shard, seq, head):
    rows, columns = shard.shape
    part = rows // seq
    mine = lax.dynamic_slice_in_dim(shard, lax.axis_index("seq") * part, part, 0)
    gathered = lax.all_gather(mine, ("seq", "head"), axis=0, tiled=True)
    gathered = gathered.reshape(seq, head, part, columns)
    return jnp.transpose(gathered, (1, 0, 2, 3)).reshape(head * rows, columns)


def to_tokens(features, head):
    tokens, width = features.shape
    pieces = features.reshape(head, tokens // head, width)
    pieces = lax.all_to_all(pieces, "head", split_axis=0, concat_axis=0, tiled=True)
    return jnp.transpose(pieces, (1, 0, 2)).reshape(tokens // head, head * width)


def per_device(
    seq,
    head,
    latent,
    modulation,
    spatial_qkv,
    spatial_out,
    temporal_qkv,
    temporal_out,
    hidden_weight,
    output_weight,
):
    patches = latent.shape[1]
    width_local = latent.shape[2]
    width = modulation.shape[1]
    own = lax.axis_index("head")
    rows = patches // (seq * head)
    frames = seq * latent.shape[0]
    share = patches // head

    ordered = jnp.transpose(latent[0].reshape(seq, head, rows, width_local), (1, 0, 2, 3))
    ordered = ordered.reshape(patches, width_local)
    full = lax.all_gather(ordered, "head", axis=1, tiled=True)
    spatial_whole = whole_weight(spatial_out, seq, head)
    query, keys, values = project_three(modulate(full, modulation, 0), spatial_qkv)
    spatial = to_tokens(spatial_attention(query, keys, values), head)
    branch = jnp.dot(spatial, spatial_whole, preferred_element_type=jnp.float32)
    mine = lax.dynamic_slice_in_dim(full, own * share, share, 0)
    stream_one = (mine.astype(jnp.float32) + modulation[2] * branch).astype(jnp.bfloat16)

    stream_one = lax.all_to_all(
        stream_one.reshape(seq, rows, width), "seq", split_axis=0, concat_axis=0, tiled=True
    ).reshape(frames * rows, width)
    temporal_in = lax.all_gather(modulate(stream_one, modulation, 3), "head", axis=0, tiled=True)
    temporal_whole = whole_weight(temporal_out, seq, head)
    query, keys, values = [
        member.reshape(head, frames, rows, width_local)
        for member in project_three(temporal_in, temporal_qkv)
    ]
    temporal = temporal_attention(query, keys, values)
    temporal = to_tokens(temporal.reshape(head * frames * rows, width_local), head)
    branch = jnp.dot(temporal, temporal_whole, preferred_element_type=jnp.float32)
    stream_two = (stream_one.astype(jnp.float32) + modulation[5] * branch).astype(jnp.bfloat16)

    hidden_in = lax.all_gather(modulate(stream_two, modulation, 6), "head", axis=0, tiled=True)
    residual = jnp.transpose(stream_two.reshape(frames * rows, head, width_local), (1, 0, 2))
    residual = lax.all_to_all(residual, "head", split_axis=0, concat_axis=0, tiled=True)
    pre_act = jnp.dot(hidden_in, hidden_weight, preferred_element_type=jnp.float32)
    hidden = jax.nn.gelu(pre_act, approximate=True).astype(jnp.bfloat16)
    partial_sums = jnp.dot(hidden, output_weight, preferred_element_type=jnp.float32)
    reduced = lax.psum_scatter(
        partial_sums.astype(jnp.bfloat16), "head", scatter_dimension=1, tiled=True
    )
    gate = lax.dynamic_slice_in_dim(modulation[8], own * width_local, width_local, 0)
    out = residual.reshape(head * frames * rows, width_local).astype(jnp.float32)
    out = (out + gate * reduced.astype(jnp.float32)).astype(jnp.bfloat16)
    out = jnp.transpose(out.reshape(head, frames, rows, width_local), (1, 0, 2, 3))
    return out.reshape(frames, head * rows, width_local)


def solution(mesh):
    in_specs = (
        P("seq", None, "head"),
        P(),
        P(None, None, "head"),
        P("head", None),
        P(None, None, "head"),
        P("head", None),
        P(None, "head"),
        P("head", None),
    )
    out_specs = P(None, "seq", "head")
    return jax.shard_map(
        functools.partial(per_device, mesh.shape["seq"], mesh.shape["head"]),
        mesh=mesh,
        in_specs=in_specs,
        out_specs=out_specs,
        check_vma=False,
    )
```
